32 devices in a mesh: blk: 8 (over z, core), grp: 4 (over y, x).
Axes of the slice: x: 2, y: 2, z: 4, core: 2. Of those that a mesh axis runs over, the one named last changes fastest.
Arguments:
- images: bfloat16 [4, 2048, 1152], P('grp', 'blk'), may hold values from -1 to 1
- texts: bfloat16 [4, 2048, 1152], P('grp', 'blk'), may hold values from -1 to 1
- labels: int32 [4, 8, 256], P('grp', 'blk'), may hold values from 0 to 255, each once within a row
- partners: int32 [2, 8], replicated, may hold values from 0 to 7, as said below
- logit_scale: float32 [], replicated, may hold values from 1 to 3
- logit_bias: float32 [], replicated, may hold values from -3 to -1
Outputs:
- image_grad: float32 [4, 2048, 1152], P('grp', 'blk')
- text_grad: float32 [4, 2048, 1152], P('grp', 'blk')
- loss: float32 [], replicated
The draws below stay inside these ranges and needn't reach their ends.
Inputs may be any that keep to these rules, and one draw needn't show every extreme that they name: Each block's labels are a permutation of its 256 text rows. partners[r, i] is block i's partner in round r: partners[r, partners[r, i]] == i and partners[r, i] != i; no two rounds pair the same two blocks.
All inputs are finite; a program needn't handle non-finite values.
Results may differ from the reference program's by a relative error of at most 0.00035.
The reference program's roundings to bfloat16 on the way (of `weight`) count: a program that leaves them out, or rounds other values in their place, can miss the bound.
Values may be sent and summed in bfloat16 or wider, within the bound.
A program may use at most 64 MiB of HBM per device.

```python
import math
import jax
import jax.numpy as jnp
from jax import lax

D = 1152
ROWS = 256
ROUNDS = 2
BLOCKS = 8
GROUPS = 4
BATCH_G = 2048


def draw_partners(key, part):
    cycle = BLOCKS - 1
    order = jax.random.permutation(jax.random.fold_in(key, 11), BLOCKS).astype(jnp.int32)
    picks = jax.random.permutation(jax.random.fold_in(key, 12), cycle)[:ROUNDS].astype(jnp.int32)
    slots = jnp.arange(BLOCKS, dtype=jnp.int32)

    def one_round(pick):
        other = jnp.where(slots == pick, cycle, (2 * pick - slots) % cycle)
        other = jnp.where(slots == cycle, pick, other).astype(jnp.int32)
        return jnp.zeros((BLOCKS,), jnp.int32).at[order].set(order[other])
    return jax.vmap(one_round)(picks).astype(jnp.int32)


def level_of(key, shape, pieces, least, top_value):
    gain, own = 1.0, jax.random.fold_in(key, 6)
    for position, parts in pieces:
        steps = jnp.exp(jax.random.uniform(jax.random.fold_in(own, position), (parts,), jnp.float32, least / len(pieces), top_value / len(pieces)))
        gain = gain * jnp.repeat(steps, shape[position] // parts).reshape([-1 if axis == position else 1 for axis in range(len(shape))])
    return gain


def gaussian(rng, dims, spread, bound, cuts=(), kind=jnp.bfloat16):
    result = jax.random.normal(rng, dims, jnp.float32) * spread
    if len(cuts) > 0:
        result = level_of(rng, dims, cuts, -0.22, 0.18) * result
    return jnp.clip(result, min=-bound, max=bound).astype(kind)


def setup_inputs(seed: int = 0) -> dict:
    seeds = jax.random.split(jax.random.key(seed), 7)
    images = gaussian(seeds[0], (GROUPS, BATCH_G, D), 0.17, 1.0, ((0, 4), (1, 8)))
    texts = gaussian(seeds[1], (GROUPS, BATCH_G, D), 0.17, 1.0, ((0, 4), (1, 8)))
    labels = jax.vmap(lambda own: jax.random.permutation(own, ROWS))(jax.random.split(seeds[2], GROUPS * BLOCKS)).reshape((GROUPS, BLOCKS, ROWS)).astype(jnp.int32)
    partners = draw_partners(jax.random.fold_in(seeds[6], 71), 0)
    logit_scale = jnp.clip(jnp.exp(jax.random.uniform(seeds[4], (), jnp.float32, math.log(1.0), math.log(3.0))), 1.0, 3.0)
    logit_bias = jnp.clip(jax.random.uniform(seeds[5], (), jnp.float32, -3.0, -1.0), -3.0, -1.0)
    return {"images": images, "texts": texts, "labels": labels, "partners": partners, "logit_scale": logit_scale, "logit_bias": logit_bias}


def pair_terms(image_rows, text_rows, positive, logit_scale, logit_bias):
    logits = logit_scale * jnp.dot(image_rows, text_rows.T, preferred_element_type=jnp.float32) + logit_bias
    signed = jnp.where(positive, jnp.float32(1.0), jnp.float32(-1.0))
    loss_sum = jnp.sum(jax.nn.softplus(-signed * logits))
    weight = (-signed * jax.nn.sigmoid(-signed * logits)).astype(jnp.bfloat16)
    image_part = logit_scale * jnp.dot(weight, text_rows, preferred_element_type=jnp.float32)
    text_part = logit_scale * jnp.dot(weight.T, image_rows, preferred_element_type=jnp.float32)
    return loss_sum, image_part, text_part


def reference(images, texts, labels, partners, logit_scale, logit_bias):
    columns = jnp.arange(ROWS, dtype=jnp.int32)
    nothing = jnp.zeros((ROWS, ROWS), dtype=bool)

    def one_group(operands):
        group_images, group_texts, group_labels = operands
        image_blocks = group_images.reshape(BLOCKS, ROWS, D)
        text_blocks = group_texts.reshape(BLOCKS, ROWS, D)
        positive = group_labels[:, :, None] == columns[None, None, :]
        losses, image_acc, text_acc = lax.map(
            lambda item: pair_terms(item[0], item[1], item[2], logit_scale, logit_bias),
            (image_blocks, text_blocks, positive))
        loss_sum = jnp.sum(losses)
        for round_index in range(ROUNDS):
            partner_row = partners[round_index].astype(jnp.int32)
            cross_loss, cross_image, cross_text = lax.map(
                lambda item: pair_terms(item[0], item[1], nothing, logit_scale, logit_bias),
                (image_blocks, text_blocks[partner_row]))
            loss_sum = loss_sum + jnp.sum(cross_loss)
            image_acc = image_acc + cross_image
            text_acc = text_acc + cross_text[partner_row]
        return loss_sum, image_acc.reshape(BATCH_G, D), text_acc.reshape(BATCH_G, D)

    group_losses, image_grad, text_grad = lax.map(one_group, (images, texts, labels))
    loss = jnp.sum(group_losses) / jnp.float32(GROUPS * BATCH_G)
    return image_grad, text_grad, loss
```

```python
import functools
import jax
import jax.numpy as jnp
from jax import lax
from jax.experimental import pallas as pl
from jax.experimental.pallas import tpu as pltpu
from jax.sharding import PartitionSpec as P

MESH = pl.DeviceIdType.MESH
CHUNK_ROWS = 16
GROUP_CHUNKS = 2
TAIL_GROUPS = 2
LINE_CHIPS = 4
VMEM_BUDGET = 48 * 1024 * 1024
VMEM_LIMIT = 56 * 1024 * 1024


def block_weights(image_rows, text_rows, positive, logit_scale, logit_bias):
    logits = (
        logit_scale * jnp.dot(image_rows, text_rows.T, preferred_element_type=jnp.float32)
        + logit_bias
    )
    signed = jnp.where(positive, jnp.float32(1.0), jnp.float32(-1.0))
    loss_sum = jnp.sum(jax.nn.softplus(-signed * logits))
    weight = (-signed * jax.nn.sigmoid(-signed * logits)).astype(jnp.bfloat16)
    return (loss_sum, weight)


def regroup(received, partner_row):
    row_count, width = received.shape
    devices = partner_row.shape[0]
    pieces = received.reshape(row_count, devices, width // devices)
    pieces = jnp.take(pieces, partner_row, axis=1)
    return pieces.reshape(row_count, width)


def spread_body(images, texts, labels, partners, logit_scale, logit_bias):
    own_images = images[0]
    own_texts = texts[0]
    row_count = own_images.shape[0]
    columns = jnp.arange(row_count, dtype=jnp.int32)
    positive = labels[0, 0][:, None] == columns[None, :]
    nothing = jnp.zeros((row_count, row_count), dtype=bool)
    loss_sum, weight = block_weights(own_images, own_texts, positive, logit_scale, logit_bias)
    image_grad = logit_scale * jnp.dot(weight, own_texts, preferred_element_type=jnp.float32)
    text_grad = logit_scale * jnp.dot(weight.T, own_images, preferred_element_type=jnp.float32)
    for round_index in range(partners.shape[0]):
        partner_row = partners[round_index]
        spread_images, spread_texts = (
            lax.all_to_all(own_images, "blk", split_axis=1, concat_axis=1, tiled=True),
            lax.all_to_all(own_texts, "blk", split_axis=1, concat_axis=1, tiled=True),
        )
        their_images, their_texts = (
            lax.all_to_all(
                regroup(spread_images, partner_row), "blk", split_axis=1, concat_axis=1, tiled=True
            ),
            lax.all_to_all(
                regroup(spread_texts, partner_row), "blk", split_axis=1, concat_axis=1, tiled=True
            ),
        )
        round_loss, weight = block_weights(
            own_images, their_texts, nothing, logit_scale, logit_bias
        )
        image_grad = image_grad + logit_scale * jnp.dot(
            weight, their_texts, preferred_element_type=jnp.float32
        )
        _, mirror = block_weights(
            their_images, own_texts, nothing, logit_scale, logit_bias
        )
        text_grad = text_grad + logit_scale * jnp.dot(
            mirror.T, their_images, preferred_element_type=jnp.float32
        )
        loss_sum = loss_sum + round_loss
    loss_all = lax.psum(loss_sum, ("blk", "grp"))
    image_count = lax.axis_size("blk") * lax.axis_size("grp") * row_count
    loss = loss_all / jnp.float32(image_count)
    return (image_grad[None], text_grad[None], loss)


def logistic_terms(value):
    small = jnp.exp(-jnp.abs(value))
    inverse = 1.0 / (1.0 + small)
    weight = jnp.where(value >= 0, inverse, small * inverse)
    return weight, jnp.maximum(value, 0.0) + jnp.log1p(small)


def rows_dot(rows, own):
    return lax.dot_general(rows, own, (((1,), (1,)), ((), ())), preferred_element_type=jnp.float32)


def weight_dot(weight, rows):
    return lax.dot_general(
        weight, rows, (((0,), (0,)), ((), ())), preferred_element_type=jnp.float32
    )


def fold(terms):
    rows, columns = terms.shape
    total = jnp.sum(terms.reshape(rows // 8, 8, columns), axis=0)
    return sum(total[:, c : c + 128] for c in range(0, columns, 128))


def exchange_kernel(
    n, groups, rounds, chunk,
    partners_ref, scale_ref, bias_ref, labels_ref, images_ref, texts_ref,
    image_acc, text_acc, loss_ref,
    own, stage, slots, loss_sum, outer_loss, loss_in, loss_sent,
    own_sem, load_sem, recv_sem, send_sem, sibling_sem, forward_sem, forwarded_sem,
    slot_send, slot_recv, outer_send, outer_recv, loss_send, loss_recv,
    seen_outer, seen_line, seen_group, seen_all, *held,
):
    rows, width = own.shape[1:]
    chunks = rows // chunk
    chips = n // 2
    me = lax.axis_index("blk")
    grp = lax.axis_index("grp")
    chip = lax.div(me, 2)
    core = lax.rem(me, 2)
    sibling = me + 1 - 2 * core
    low = chip < chips // 2
    outer = jnp.logical_or(chip == 0, chip == chips - 1)
    inner = jnp.logical_not(outer)
    hub = chip == 0
    near = jnp.where(low, 0, chips - 1)
    far = chips - 1 - near
    beside = jnp.where(low, 1, chips - 2)
    across = chips - 1 - beside
    inner_count = n - 4
    scale = scale_ref[0]
    bias = bias_ref[0]

    def part(k):
        return pl.ds(k * chunk, chunk)

    def own_loads(k):
        return [
            pltpu.make_async_copy(ref.at[0, part(k)], own.at[i, part(k)], own_sem.at[k, i])
            for i, ref in enumerate((images_ref, texts_ref))
        ]

    def held_loads(k):
        return [
            pltpu.make_async_copy(ref.at[0, part(k)], held[k].at[me, i], load_sem.at[k, i])
            for i, ref in enumerate((images_ref, texts_ref))
        ]

    def each(copies, act):
        for copy in copies:
            act(copy)

    for k in range(chunks):
        each(own_loads(k), lambda copy: copy.start())
    for k in range(chunks):
        pl.when(jnp.logical_and(inner, core == k % 2))(
            lambda k=k: each(held_loads(k), lambda copy: copy.start())
        )

    barrier = pltpu.get_barrier_semaphore()

    def signal(semaphore, **device):
        pl.semaphore_signal(semaphore, inc=1, device_id=device, device_id_type=MESH)

    signal(barrier, blk=sibling)

    @pl.when(inner)
    def _():
        for other in (across, near, far):
            for c in range(2):
                signal(barrier, blk=2 * other + c)
        pl.semaphore_wait(barrier, 5)

    @pl.when(outer)
    def _():
        for c in range(2):
            signal(barrier, blk=2 * beside + c)

    @pl.when(hub)
    def _():
        for step in range(1, groups):
            signal(barrier, grp=lax.rem(grp + step, groups))
        pl.semaphore_wait(barrier, 5 + groups - 1)

    pl.when(jnp.logical_and(outer, jnp.logical_not(hub)))(lambda: pl.semaphore_wait(barrier, 5))

    def remote(src, dst, send, recv, **device):
        return pltpu.make_async_remote_copy(
            src_ref=src, dst_ref=dst, send_sem=send, recv_sem=recv,
            device_id=device, device_id_type=MESH,
        )

    def send_rows(k, target, send):
        return remote(own.at[:, part(k)], held[k].at[me], send, recv_sem.at[k], blk=target)

    def rows_arrived(k):
        block = held[k].at[pl.ds(0, n - 1)]
        return remote(block, block, send_sem.at[0], recv_sem.at[k], blk=sibling)

    def all_rows_sent(send):
        return remote(own, own, send, recv_sem.at[0], blk=sibling)

    def half_rows_sent(send):
        return remote(own.at[0], own.at[0], send, recv_sem.at[0], blk=sibling)

    def forward(k):
        return remote(held[k], held[k], forward_sem.at[k], forwarded_sem.at[k], blk=sibling)

    def slot_copy(k, c):
        return remote(
            stage.at[k // 2, c], slots.at[k], slot_send, slot_recv.at[k], blk=2 * near + c
        )

    def outer_loss_copy():
        return remote(
            outer_loss.at[0], outer_loss.at[1], outer_send, outer_recv, blk=2 * beside + core
        )

    def loss_copy(index, blk, group):
        slot = loss_in.at[index]
        return remote(slot, slot, loss_send, loss_recv, blk=blk, grp=group)

    def losses_arrived(count):
        slot = loss_in.at[pl.ds(0, count)]
        return remote(slot, slot, loss_send, loss_recv, blk=sibling)

    def losses_sent():
        return remote(loss_sent, loss_sent, loss_send, loss_recv, blk=sibling)

    def own_pair():
        logits = scale * rows_dot(own[1], own[0]) + bias
        positive = lax.broadcasted_iota(jnp.int32, logits.shape, 0) == labels_ref[0]
        signed = jnp.where(positive, -1.0, 1.0)
        weight, terms = logistic_terms(signed * logits)
        weight = (signed * weight).astype(jnp.bfloat16)
        loss_sum[...] = fold(terms)
        image_acc[0] = weight_dot(weight, own[1])
        text_acc[0] = jnp.dot(weight, own[0], preferred_element_type=jnp.float32)

    def add_pairs(their_images, their_texts, with_loss):
        weight, terms = logistic_terms(scale * rows_dot(their_texts, own[0]) + bias)
        if with_loss:
            loss_sum[...] += fold(terms)
        mirror, _ = logistic_terms(scale * rows_dot(their_images, own[1]) + bias)
        image_acc[0] += weight_dot(weight.astype(jnp.bfloat16), their_texts)
        text_acc[0] += weight_dot(mirror.astype(jnp.bfloat16), their_images)

    def joined(pieces):
        return jnp.concatenate(pieces, axis=0)

    group_list = [
        list(range(k, k + GROUP_CHUNKS)) for k in range(0, chunks, GROUP_CHUNKS)
    ]
    tail = [k for members in group_list[-TAIL_GROUPS:] for k in members]

    @pl.when(outer)
    def _():
        for k in range(chunks):
            each(own_loads(k), lambda copy: copy.wait())
            send_rows(k, 2 * across + k % 2, send_sem.at[0]).start()
            send_rows(k, 2 * beside + k % 2, send_sem.at[1]).start()
        for other in (beside, across):
            signal(seen_outer, blk=2 * other + core)
        own_pair()

        def add_slots(members, with_loss):
            for k in members:
                slot_copy(k, 0).wait_recv()
            found = [
                joined([slots[k, r, i] for r in range(rounds) for k in members])
                for i in range(2)
            ]
            add_pairs(found[0], found[1], with_loss)

        for members in group_list[:-TAIL_GROUPS]:
            add_slots(members, True)
            if members[0] == 0:
                @pl.when(hub)
                def _():
                    pl.semaphore_wait(seen_line, 1)
                    for step in range(1, groups):
                        signal(seen_group, grp=lax.rem(grp + step, groups))
                    pl.semaphore_wait(seen_group, groups - 1)
                    for other in (beside, across):
                        signal(seen_all, blk=2 * other + core)

        outer_loss[0] = jnp.sum(loss_sum[...], axis=0, keepdims=True)
        outer_loss_copy().start()
        for members in group_list[-TAIL_GROUPS:-1]:
            add_slots(members, False)
        all_rows_sent(send_sem.at[0]).wait_send()
        all_rows_sent(send_sem.at[1]).wait_send()
        outer_loss_copy().wait_send()
        for k in group_list[-1]:
            add_slots([k], False)
        losses_arrived(inner_count * groups).wait_recv()

    @pl.when(inner)
    def _():
        for k in range(chunks):
            each(own_loads(k), lambda copy: copy.wait())
            send_rows(k, 2 * across + k % 2, send_sem.at[0]).start()
            pl.when(core != k % 2)(
                lambda k=k: send_rows(k, sibling, sibling_sem).start()
            )
        own_pair()

        def select(k):
            each(held_loads(k), lambda copy: copy.wait())
            rows_arrived(k).wait_recv()
            for c in range(2):
                for r in range(rounds):
                    stage[k // 2, c, r] = held[k][partners_ref[r, 2 * near + c]]
                slot_copy(k, c).start()
            forward(k).start()

        def add_held(members):
            for c in range(2):
                @pl.when(core == c)
                def _():
                    for k in members:
                        if k % 2 == c:
                            select(k)
                    for k in members:
                        if k % 2 != c:
                            forward(k).wait_recv()
            found = [
                joined([
                    held[k][partners_ref[r, me], i] for r in range(rounds) for k in members
                ])
                for i in range(2)
            ]
            add_pairs(found[0], found[1], True)

        for members in group_list:
            add_held(members)
            if members[0] == 0:
                pl.semaphore_wait(seen_outer, 2)
                pl.when(low)(lambda: signal(seen_line, blk=2 * near + core))

        end_images = [
            joined([held[k][2 * near + c, 0] for k in range(chunks)]) for c in range(2)
        ]
        for parity in range(2):
            @pl.when(core == parity)
            def _():
                mine = [k for k in tail if k % 2 == parity]
                for c in range(2):
                    texts = joined([stage[k // 2, c, r, 1] for r in range(rounds) for k in mine])
                    _, terms = logistic_terms(scale * rows_dot(texts, end_images[c]) + bias)
                    loss_sum[...] += fold(terms)

        outer_loss_copy().wait_recv()
        pl.semaphore_wait(seen_all, 1)
        index = grp * inner_count + me - 2
        loss_in[index] = jnp.sum(loss_sum[...], axis=0, keepdims=True) + outer_loss[1]
        for step in range(groups):
            for hop in range(n):
                if step + hop > 0:
                    loss_copy(
                        index, lax.rem(me + hop, n), lax.rem(grp + step, groups)
                    ).start()
        for k in range(chunks):
            pl.when(core == k % 2)(lambda k=k: forward(k).wait_send())
        all_rows_sent(send_sem.at[0]).wait_send()
        half_rows_sent(sibling_sem).wait_send()
        remote(stage, stage, slot_send, slot_recv.at[0], blk=sibling).wait_send()
        losses_sent().wait_send()
        losses_arrived(inner_count * groups - 1).wait_recv()

    total = loss_in[0]
    for at in range(1, inner_count * groups):
        total = total + loss_in[at]
    loss_ref[0, 0] = jnp.sum(total) / jnp.float32(n * groups * rows)


def line_body(n, groups, images, texts, labels, partners, logit_scale, logit_bias):
    _, rows, width = images.shape
    rounds = partners.shape[0]
    chunk = CHUNK_ROWS
    chunks = rows // chunk
    vmem = pl.BlockSpec(memory_space=pltpu.VMEM)
    smem = pl.BlockSpec(memory_space=pltpu.SMEM)
    hbm = pl.BlockSpec(memory_space=pl.ANY)
    dma = pltpu.SemaphoreType.DMA
    regular = pltpu.SemaphoreType.REGULAR
    grad = jax.ShapeDtypeStruct(images.shape, jnp.float32)
    inner_count = n - 4
    image_grad, text_grad, loss = pl.pallas_call(
        functools.partial(exchange_kernel, n, groups, rounds, chunk),
        out_shape=(grad, grad, jax.ShapeDtypeStruct((1, 1), jnp.float32)),
        in_specs=[smem, smem, smem, vmem, hbm, hbm],
        out_specs=(vmem, vmem, smem),
        scratch_shapes=[
            pltpu.VMEM((2, rows, width), images.dtype),
            pltpu.VMEM((chunks // 2, 2, rounds, 2, chunk, width), images.dtype),
            pltpu.VMEM((chunks, rounds, 2, chunk, width), images.dtype),
            pltpu.VMEM((8, 128), jnp.float32),
            pltpu.VMEM((2, 1, 128), jnp.float32),
            pltpu.VMEM((inner_count * groups, 1, 128), jnp.float32),
            pltpu.VMEM((n * groups - 1, 1, 128), jnp.float32),
            dma((chunks, 2)),
            dma((chunks, 2)),
            dma((chunks,)),
            dma((2,)),
            dma,
            dma((chunks,)),
            dma((chunks,)),
            dma,
            dma((chunks,)),
            dma,
            dma,
            dma,
            dma,
            regular,
            regular,
            regular,
            regular,
        ]
        + [pltpu.VMEM((n, 2, chunk, width), images.dtype) for _ in range(chunks)],
        compiler_params=pltpu.CompilerParams(
            collective_id=0, has_side_effects=True, vmem_limit_bytes=VMEM_LIMIT
        ),
    )(partners, logit_scale.reshape(1), logit_bias.reshape(1), labels, images, texts)
    return logit_scale * image_grad, logit_scale * text_grad, loss.reshape(())


def solution(mesh):
    in_specs = (P("grp", "blk", None), P("grp", "blk", None), P("grp", "blk", None), P(), P(), P())
    out_specs = (P("grp", "blk", None), P("grp", "blk", None), P())
    n, groups = mesh.shape["blk"], mesh.shape["grp"]

    def body(images, texts, labels, partners, logit_scale, logit_bias):
        _, rows, width = images.shape
        rounds = partners.shape[0]
        block = 2 * rows * width * images.dtype.itemsize
        needed = block * (n + 3 * rounds + 1) + 2 * rows * width * 4
        fits = needed <= VMEM_BUDGET and n == 2 * LINE_CHIPS and groups > 1
        if fits and rows % 128 == 0 and width % 128 == 0:
            return line_body(
                n, groups, images, texts, labels, partners, logit_scale, logit_bias
            )
        return spread_body(images, texts, labels, partners, logit_scale, logit_bias)

    return jax.shard_map(body, mesh=mesh, in_specs=in_specs, out_specs=out_specs, check_vma=False)
```

```python
import functools
import jax
import jax.numpy as jnp
from jax import lax
from jax.experimental import pallas as pl
from jax.experimental.pallas import tpu as pltpu
from jax.sharding import PartitionSpec as P

MESH = pl.DeviceIdType.MESH
CHUNK_ROWS = 16
GROUP_CHUNKS = 2
TAIL_GROUPS = 2
LINE_CHIPS = 4
VMEM_BUDGET = 48 * 1024 * 1024
VMEM_LIMIT = 32 * 1024 * 1024
FINISH_LIMIT = 16 * 1024 * 1024


def block_weights(image_rows, text_rows, positive, logit_scale, logit_bias):
    logits = (
        logit_scale * jnp.dot(image_rows, text_rows.T, preferred_element_type=jnp.float32)
        + logit_bias
    )
    signed = jnp.where(positive, jnp.float32(1.0), jnp.float32(-1.0))
    loss_sum = jnp.sum(jax.nn.softplus(-signed * logits))
    weight = (-signed * jax.nn.sigmoid(-signed * logits)).astype(jnp.bfloat16)
    return (loss_sum, weight)


def regroup(received, partner_row):
    row_count, width = received.shape
    devices = partner_row.shape[0]
    pieces = received.reshape(row_count, devices, width // devices)
    pieces = jnp.take(pieces, partner_row, axis=1)
    return pieces.reshape(row_count, width)


def spread_body(images, texts, labels, partners, logit_scale, logit_bias):
    own_images = images[0]
    own_texts = texts[0]
    row_count = own_images.shape[0]
    columns = jnp.arange(row_count, dtype=jnp.int32)
    positive = labels[0, 0][:, None] == columns[None, :]
    nothing = jnp.zeros((row_count, row_count), dtype=bool)
    loss_sum, weight = block_weights(own_images, own_texts, positive, logit_scale, logit_bias)
    image_grad = logit_scale * jnp.dot(weight, own_texts, preferred_element_type=jnp.float32)
    text_grad = logit_scale * jnp.dot(weight.T, own_images, preferred_element_type=jnp.float32)
    for round_index in range(partners.shape[0]):
        partner_row = partners[round_index]
        spread_images, spread_texts = (
            lax.all_to_all(own_images, "blk", split_axis=1, concat_axis=1, tiled=True),
            lax.all_to_all(own_texts, "blk", split_axis=1, concat_axis=1, tiled=True),
        )
        their_images, their_texts = (
            lax.all_to_all(
                regroup(spread_images, partner_row), "blk", split_axis=1, concat_axis=1, tiled=True
            ),
            lax.all_to_all(
                regroup(spread_texts, partner_row), "blk", split_axis=1, concat_axis=1, tiled=True
            ),
        )
        round_loss, weight = block_weights(
            own_images, their_texts, nothing, logit_scale, logit_bias
        )
        image_grad = image_grad + logit_scale * jnp.dot(
            weight, their_texts, preferred_element_type=jnp.float32
        )
        _, mirror = block_weights(
            their_images, own_texts, nothing, logit_scale, logit_bias
        )
        text_grad = text_grad + logit_scale * jnp.dot(
            mirror.T, their_images, preferred_element_type=jnp.float32
        )
        loss_sum = loss_sum + round_loss
    loss_all = lax.psum(loss_sum, ("blk", "grp"))
    image_count = lax.axis_size("blk") * lax.axis_size("grp") * row_count
    loss = loss_all / jnp.float32(image_count)
    return (image_grad[None], text_grad[None], loss)


def logistic_terms(value):
    small = jnp.exp(-jnp.abs(value))
    inverse = 1.0 / (1.0 + small)
    weight = jnp.where(value >= 0, inverse, small * inverse)
    return weight, jnp.maximum(value, 0.0) + jnp.log1p(small)


def rows_dot(rows, own):
    return lax.dot_general(rows, own, (((1,), (1,)), ((), ())), preferred_element_type=jnp.float32)


def weight_dot(weight, rows):
    return lax.dot_general(
        weight, rows, (((0,), (0,)), ((), ())), preferred_element_type=jnp.float32
    )


def fold(terms):
    rows, columns = terms.shape
    total = jnp.sum(terms.reshape(rows // 8, 8, columns), axis=0)
    return sum(total[:, c : c + 128] for c in range(0, columns, 128))


def exchange_kernel(
    n, groups, rounds, chunk,
    partners_in, scale_ref, bias_ref, labels_in, images_ref, texts_ref,
    image_acc, text_acc, loss_ref,
    partners_ref, labels_ref, small_sem, own, stage, slots, loss_sum, outer_loss, loss_in, loss_sent,
    own_sem, load_sem, recv_sem, send_sem, sibling_sem, forward_sem, forwarded_sem,
    slot_send, slot_recv, outer_send, outer_recv, loss_send, loss_recv,
    seen_outer, seen_line, seen_group, seen_all, *held,
):
    rows, width = own.shape[1:]
    chunks = rows // chunk
    chips = n // 2
    me = lax.axis_index("blk")
    grp = lax.axis_index("grp")
    chip = lax.div(me, 2)
    core = lax.rem(me, 2)
    sibling = me + 1 - 2 * core
    low = chip < chips // 2
    outer = jnp.logical_or(chip == 0, chip == chips - 1)
    inner = jnp.logical_not(outer)
    hub = chip == 0
    near = jnp.where(low, 0, chips - 1)
    far = chips - 1 - near
    beside = jnp.where(low, 1, chips - 2)
    across = chips - 1 - beside
    inner_count = n - 4
    def part(k):
        return pl.ds(k * chunk, chunk)

    def own_loads(k):
        return [
            pltpu.make_async_copy(ref.at[0, part(k)], own.at[i, part(k)], own_sem.at[k, i])
            for i, ref in enumerate((images_ref, texts_ref))
        ]

    def held_loads(k):
        return [
            pltpu.make_async_copy(ref.at[0, part(k)], held[k].at[me, i], load_sem.at[k, i])
            for i, ref in enumerate((images_ref, texts_ref))
        ]

    def each(copies, act):
        for copy in copies:
            act(copy)

    small = [
        pltpu.make_async_copy(src, dst, small_sem.at[i])
        for i, (src, dst) in enumerate((
            (labels_in.at[0], labels_ref), (partners_in, partners_ref),
        ))
    ]
    for k in range(chunks):
        each(own_loads(k), lambda copy: copy.start())
    each(small, lambda copy: copy.start())
    for k in range(chunks):
        pl.when(jnp.logical_and(inner, core == k % 2))(
            lambda k=k: each(held_loads(k), lambda copy: copy.start())
        )

    barrier = pltpu.get_barrier_semaphore()

    def signal(semaphore, **device):
        pl.semaphore_signal(semaphore, inc=1, device_id=device, device_id_type=MESH)

    signal(barrier, blk=sibling)

    @pl.when(inner)
    def _():
        for other in (across, near, far):
            for c in range(2):
                signal(barrier, blk=2 * other + c)
        pl.semaphore_wait(barrier, 5)

    @pl.when(outer)
    def _():
        for c in range(2):
            signal(barrier, blk=2 * beside + c)

    @pl.when(hub)
    def _():
        for step in range(1, groups):
            signal(barrier, grp=lax.rem(grp + step, groups))
        pl.semaphore_wait(barrier, 5 + groups - 1)

    pl.when(jnp.logical_and(outer, jnp.logical_not(hub)))(lambda: pl.semaphore_wait(barrier, 5))

    def remote(src, dst, send, recv, **device):
        return pltpu.make_async_remote_copy(
            src_ref=src, dst_ref=dst, send_sem=send, recv_sem=recv,
            device_id=device, device_id_type=MESH,
        )

    def send_rows(k, target, send):
        return remote(own.at[:, part(k)], held[k].at[me], send, recv_sem.at[k], blk=target)

    def rows_arrived(k):
        block = held[k].at[pl.ds(0, n - 1)]
        return remote(block, block, send_sem.at[0], recv_sem.at[k], blk=sibling)

    def all_rows_sent(send):
        return remote(own, own, send, recv_sem.at[0], blk=sibling)

    def half_rows_sent(send):
        return remote(own.at[0], own.at[0], send, recv_sem.at[0], blk=sibling)

    def forward(k):
        return remote(held[k], held[k], forward_sem.at[k], forwarded_sem.at[k], blk=sibling)

    def slot_copy(k, c):
        return remote(
            stage.at[k // 2, c], slots.at[k], slot_send, slot_recv.at[k], blk=2 * near + c
        )

    def outer_loss_copy():
        return remote(
            outer_loss.at[0], outer_loss.at[1], outer_send, outer_recv, blk=2 * beside + core
        )

    def loss_copy(index, blk, group):
        slot = loss_in.at[index]
        return remote(slot, slot, loss_send, loss_recv, blk=blk, grp=group)

    def losses_arrived(count):
        slot = loss_in.at[pl.ds(0, count)]
        return remote(slot, slot, loss_send, loss_recv, blk=sibling)

    def losses_sent():
        return remote(loss_sent, loss_sent, loss_send, loss_recv, blk=sibling)

    def own_pair():
        scale, bias = scale_ref[...], bias_ref[...]
        logits = scale * rows_dot(own[1], own[0]) + bias
        positive = lax.broadcasted_iota(jnp.int32, logits.shape, 0) == labels_ref[...]
        signed = jnp.where(positive, -1.0, 1.0)
        weight, terms = logistic_terms(signed * logits)
        weight = (signed * weight).astype(jnp.bfloat16)
        loss_sum[...] = fold(terms)
        image_acc[0] = weight_dot(weight, own[1])
        text_acc[0] = jnp.dot(weight, own[0], preferred_element_type=jnp.float32)

    def add_pairs(their_images, their_texts, with_loss, last):
        scale, bias = scale_ref[...], bias_ref[...]
        weight, terms = logistic_terms(scale * rows_dot(their_texts, own[0]) + bias)
        if with_loss:
            loss_sum[...] += fold(terms)
        mirror, _ = logistic_terms(scale * rows_dot(their_images, own[1]) + bias)
        image_sum = image_acc[0] + weight_dot(weight.astype(jnp.bfloat16), their_texts)
        text_sum = text_acc[0] + weight_dot(mirror.astype(jnp.bfloat16), their_images)
        image_acc[0] = scale * image_sum if last else image_sum
        text_acc[0] = scale * text_sum if last else text_sum

    def joined(pieces):
        return jnp.concatenate(pieces, axis=0)

    group_list = [
        list(range(k, k + GROUP_CHUNKS)) for k in range(0, chunks, GROUP_CHUNKS)
    ]
    tail = [k for members in group_list[-TAIL_GROUPS:] for k in members]

    @pl.when(outer)
    def _():
        for k in range(chunks):
            each(own_loads(k), lambda copy: copy.wait())
            send_rows(k, 2 * across + k % 2, send_sem.at[0]).start()
            send_rows(k, 2 * beside + k % 2, send_sem.at[1]).start()
        for other in (beside, across):
            signal(seen_outer, blk=2 * other + core)
        each(small, lambda copy: copy.wait())
        own_pair()

        def add_slots(members, with_loss, last=False):
            for k in members:
                slot_copy(k, 0).wait_recv()
            found = [
                joined([slots[k, r, i] for r in range(rounds) for k in members])
                for i in range(2)
            ]
            add_pairs(found[0], found[1], with_loss, last)

        for members in group_list[:-TAIL_GROUPS]:
            add_slots(members, True)
            if members[0] == 0:
                @pl.when(hub)
                def _():
                    pl.semaphore_wait(seen_line, 1)
                    for step in range(1, groups):
                        signal(seen_group, grp=lax.rem(grp + step, groups))
                    pl.semaphore_wait(seen_group, groups - 1)
                    for other in (beside, across):
                        signal(seen_all, blk=2 * other + core)

        outer_loss[0] = jnp.sum(loss_sum[...], axis=0, keepdims=True)
        outer_loss_copy().start()
        for members in group_list[-TAIL_GROUPS:-1]:
            add_slots(members, False)
        all_rows_sent(send_sem.at[0]).wait_send()
        all_rows_sent(send_sem.at[1]).wait_send()
        outer_loss_copy().wait_send()
        for k in group_list[-1]:
            add_slots([k], False, k == chunks - 1)
        losses_arrived(inner_count * groups).wait_recv()

    @pl.when(inner)
    def _():
        for k in range(chunks):
            each(own_loads(k), lambda copy: copy.wait())
            send_rows(k, 2 * across + k % 2, send_sem.at[0]).start()
            pl.when(core != k % 2)(
                lambda k=k: send_rows(k, sibling, sibling_sem).start()
            )
        each(small, lambda copy: copy.wait())
        own_pair()

        def select(k):
            each(held_loads(k), lambda copy: copy.wait())
            rows_arrived(k).wait_recv()
            for c in range(2):
                for r in range(rounds):
                    stage[k // 2, c, r] = held[k][partners_ref[r, 2 * near + c]]
                slot_copy(k, c).start()
            forward(k).start()

        def add_held(members):
            for c in range(2):
                @pl.when(core == c)
                def _():
                    for k in members:
                        if k % 2 == c:
                            select(k)
                    for k in members:
                        if k % 2 != c:
                            forward(k).wait_recv()
            found = [
                joined([
                    held[k][partners_ref[r, me], i] for r in range(rounds) for k in members
                ])
                for i in range(2)
            ]
            add_pairs(found[0], found[1], True, members[-1] == chunks - 1)

        for members in group_list:
            add_held(members)
            if members[0] == 0:
                pl.semaphore_wait(seen_outer, 2)
                pl.when(low)(lambda: signal(seen_line, blk=2 * near + core))

        end_images = [
            joined([held[k][2 * near + c, 0] for k in range(chunks)]) for c in range(2)
        ]
        for parity in range(2):
            @pl.when(core == parity)
            def _():
                mine = [k for k in tail if k % 2 == parity]
                for c in range(2):
                    texts = joined([stage[k // 2, c, r, 1] for r in range(rounds) for k in mine])
                    logits = scale_ref[...] * rows_dot(texts, end_images[c]) + bias_ref[...]
                    _, terms = logistic_terms(logits)
                    loss_sum[...] += fold(terms)

        outer_loss_copy().wait_recv()
        pl.semaphore_wait(seen_all, 1)
        index = grp * inner_count + me - 2
        loss_in[index] = jnp.sum(loss_sum[...], axis=0, keepdims=True) + outer_loss[1]
        for step in range(groups):
            for hop in range(n):
                if step + hop > 0:
                    loss_copy(
                        index, lax.rem(me + hop, n), lax.rem(grp + step, groups)
                    ).start()
        for k in range(chunks):
            pl.when(core == k % 2)(lambda k=k: forward(k).wait_send())
        all_rows_sent(send_sem.at[0]).wait_send()
        half_rows_sent(sibling_sem).wait_send()
        remote(stage, stage, slot_send, slot_recv.at[0], blk=sibling).wait_send()
        losses_sent().wait_send()
        losses_arrived(inner_count * groups - 1).wait_recv()

    total = loss_in[0]
    for at in range(1, inner_count * groups):
        total = total + loss_in[at]
    loss_ref[...] = total


def finish_kernel(
    image_count, image_in, text_in, loss_in, image_out, text_out, loss_out, loss_cell, sems
):
    copies = [
        pltpu.make_async_copy(image_in, image_out, sems.at[0]),
        pltpu.make_async_copy(text_in, text_out, sems.at[1]),
        pltpu.make_async_copy(loss_cell, loss_out, sems.at[2]),
    ]
    copies[0].start()
    copies[1].start()
    loss_cell[0, 0] = jnp.sum(loss_in[...]) / jnp.float32(image_count)
    copies[2].start()
    for copy in copies:
        copy.wait()


def keep(array):
    return pltpu.with_memory_space_constraint(array, pltpu.HBM)


def line_body(n, groups, images, texts, labels, partners, logit_scale, logit_bias):
    _, rows, width = images.shape
    rounds = partners.shape[0]
    chunk = CHUNK_ROWS
    chunks = rows // chunk
    vmem = pl.BlockSpec(memory_space=pltpu.VMEM)
    smem = pl.BlockSpec(memory_space=pltpu.SMEM)
    hbm = pl.BlockSpec(memory_space=pl.ANY)
    dma = pltpu.SemaphoreType.DMA
    regular = pltpu.SemaphoreType.REGULAR
    grad = jax.ShapeDtypeStruct(images.shape, jnp.float32)
    inner_count = n - 4
    image_sum, text_sum, loss_sum = pl.pallas_call(
        functools.partial(exchange_kernel, n, groups, rounds, chunk),
        out_shape=(grad, grad, jax.ShapeDtypeStruct((1, 128), jnp.float32)),
        in_specs=[hbm, smem, smem, hbm, hbm, hbm],
        out_specs=(vmem, vmem, vmem),
        scratch_shapes=[
            pltpu.SMEM((rounds, n), jnp.int32),
            pltpu.VMEM((1, rows), jnp.int32),
            dma((4,)),
            pltpu.VMEM((2, rows, width), images.dtype),
            pltpu.VMEM((chunks // 2, 2, rounds, 2, chunk, width), images.dtype),
            pltpu.VMEM((chunks, rounds, 2, chunk, width), images.dtype),
            pltpu.VMEM((8, 128), jnp.float32),
            pltpu.VMEM((2, 1, 128), jnp.float32),
            pltpu.VMEM((inner_count * groups, 1, 128), jnp.float32),
            pltpu.VMEM((n * groups - 1, 1, 128), jnp.float32),
            dma((chunks, 2)),
            dma((chunks, 2)),
            dma((chunks,)),
            dma((2,)),
            dma,
            dma((chunks,)),
            dma((chunks,)),
            dma,
            dma((chunks,)),
            dma,
            dma,
            dma,
            dma,
            regular,
            regular,
            regular,
            regular,
        ]
        + [pltpu.VMEM((n, 2, chunk, width), images.dtype) for _ in range(chunks)],
        compiler_params=pltpu.CompilerParams(
            collective_id=0, has_side_effects=True, vmem_limit_bytes=VMEM_LIMIT
        ),
    )(
        keep(partners), logit_scale, logit_bias,
        keep(labels), keep(images), keep(texts),
    )
    image_grad, text_grad, loss = pl.pallas_call(
        functools.partial(finish_kernel, n * groups * rows),
        out_shape=(grad, grad, jax.ShapeDtypeStruct((1, 1), jnp.float32)),
        in_specs=[vmem, vmem, vmem],
        out_specs=(hbm, hbm, hbm),
        scratch_shapes=[pltpu.SMEM((1, 1), jnp.float32), dma((3,))],
        compiler_params=pltpu.CompilerParams(vmem_limit_bytes=FINISH_LIMIT),
    )(image_sum, text_sum, loss_sum)
    return image_grad, text_grad, loss.reshape(())


def solution(mesh):
    in_specs = (P("grp", "blk", None), P("grp", "blk", None), P("grp", "blk", None), P(), P(), P())
    out_specs = (P("grp", "blk", None), P("grp", "blk", None), P())
    n, groups = mesh.shape["blk"], mesh.shape["grp"]

    def body(images, texts, labels, partners, logit_scale, logit_bias):
        _, rows, width = images.shape
        rounds = partners.shape[0]
        block = 2 * rows * width * images.dtype.itemsize
        needed = block * (n + 3 * rounds + 1) + 2 * rows * width * 4
        fits = needed <= VMEM_BUDGET and n == 2 * LINE_CHIPS and groups > 1
        if fits and rows % 128 == 0 and width % 128 == 0:
            return line_body(
                n, groups, images, texts, labels, partners, logit_scale, logit_bias
            )
        return spread_body(images, texts, labels, partners, logit_scale, logit_bias)

    return jax.shard_map(body, mesh=mesh, in_specs=in_specs, out_specs=out_specs, check_vma=False)
```

```python
import functools
import jax
import jax.numpy as jnp
from jax import lax
from jax.experimental import pallas as pl
from jax.experimental.pallas import tpu as pltpu
from jax.sharding import PartitionSpec as P

MESH = pl.DeviceIdType.MESH
CHUNK_ROWS = 16
GROUP_CHUNKS = 4
AHEAD_CHUNKS = 12
LINE_CHIPS = 4
VMEM_BUDGET = 48 * 1024 * 1024
VMEM_LIMIT = 32 * 1024 * 1024
FINISH_LIMIT = 16 * 1024 * 1024
FINISH_STEPS = 2


def block_weights(image_rows, text_rows, positive, logit_scale, logit_bias):
    logits = (
        logit_scale * jnp.dot(image_rows, text_rows.T, preferred_element_type=jnp.float32)
        + logit_bias
    )
    signed = jnp.where(positive, jnp.float32(1.0), jnp.float32(-1.0))
    loss_sum = jnp.sum(jax.nn.softplus(-signed * logits))
    weight = (-signed * jax.nn.sigmoid(-signed * logits)).astype(jnp.bfloat16)
    return (loss_sum, weight)


def regroup(received, partner_row):
    row_count, width = received.shape
    devices = partner_row.shape[0]
    pieces = received.reshape(row_count, devices, width // devices)
    pieces = jnp.take(pieces, partner_row, axis=1)
    return pieces.reshape(row_count, width)


def spread_body(images, texts, labels, partners, logit_scale, logit_bias):
    own_images = images[0]
    own_texts = texts[0]
    row_count = own_images.shape[0]
    columns = jnp.arange(row_count, dtype=jnp.int32)
    positive = labels[0, 0][:, None] == columns[None, :]
    nothing = jnp.zeros((row_count, row_count), dtype=bool)
    loss_sum, weight = block_weights(own_images, own_texts, positive, logit_scale, logit_bias)
    image_grad = logit_scale * jnp.dot(weight, own_texts, preferred_element_type=jnp.float32)
    text_grad = logit_scale * jnp.dot(weight.T, own_images, preferred_element_type=jnp.float32)
    for round_index in range(partners.shape[0]):
        partner_row = partners[round_index]
        spread_images, spread_texts = (
            lax.all_to_all(own_images, "blk", split_axis=1, concat_axis=1, tiled=True),
            lax.all_to_all(own_texts, "blk", split_axis=1, concat_axis=1, tiled=True),
        )
        their_images, their_texts = (
            lax.all_to_all(
                regroup(spread_images, partner_row), "blk", split_axis=1, concat_axis=1, tiled=True
            ),
            lax.all_to_all(
                regroup(spread_texts, partner_row), "blk", split_axis=1, concat_axis=1, tiled=True
            ),
        )
        round_loss, weight = block_weights(
            own_images, their_texts, nothing, logit_scale, logit_bias
        )
        image_grad = image_grad + logit_scale * jnp.dot(
            weight, their_texts, preferred_element_type=jnp.float32
        )
        _, mirror = block_weights(
            their_images, own_texts, nothing, logit_scale, logit_bias
        )
        text_grad = text_grad + logit_scale * jnp.dot(
            mirror.T, their_images, preferred_element_type=jnp.float32
        )
        loss_sum = loss_sum + round_loss
    loss_all = lax.psum(loss_sum, ("blk", "grp"))
    image_count = lax.axis_size("blk") * lax.axis_size("grp") * row_count
    loss = loss_all / jnp.float32(image_count)
    return (image_grad[None], text_grad[None], loss)


def logistic_terms(value):
    small = jnp.exp(-jnp.abs(value))
    inverse = 1.0 / (1.0 + small)
    weight = jnp.where(value >= 0, inverse, small * inverse)
    return weight, jnp.maximum(value, 0.0) + jnp.log1p(small)


def rows_dot(rows, own):
    return lax.dot_general(rows, own, (((1,), (1,)), ((), ())), preferred_element_type=jnp.float32)


def weight_dot(weight, rows):
    return lax.dot_general(
        weight, rows, (((0,), (0,)), ((), ())), preferred_element_type=jnp.float32
    )


def fold(terms):
    rows, columns = terms.shape
    total = jnp.sum(terms.reshape(rows // 8, 8, columns), axis=0)
    return sum(total[:, c : c + 128] for c in range(0, columns, 128))


def exchange_kernel(
    n, groups, rounds, chunk,
    partners_in, scale_ref, bias_ref, labels_in, images_ref, texts_ref,
    image_acc, text_acc, tail_weight, tail_rows, loss_ref,
    partners_ref, labels_ref, small_sem, own, stage, slots, loss_sum, outer_loss, loss_in, loss_sent,
    own_sem, load_sem, recv_sem, send_sem, sibling_sem, forward_sem, forwarded_sem,
    slot_send, slot_recv, outer_send, outer_recv, loss_send, loss_recv,
    seen_outer, seen_line, seen_group, seen_all, *held,
):
    rows = own.shape[1]
    half = rows // chunk
    chunks = 2 * half
    chips = n // 2
    me = lax.axis_index("blk")
    grp = lax.axis_index("grp")
    chip = lax.div(me, 2)
    core = lax.rem(me, 2)
    sibling = me + 1 - 2 * core
    low = chip < chips // 2
    outer = jnp.logical_or(chip == 0, chip == chips - 1)
    inner = jnp.logical_not(outer)
    hub = chip == 0
    near = jnp.where(low, 0, chips - 1)
    far = chips - 1 - near
    beside = jnp.where(low, 1, chips - 2)
    across = chips - 1 - beside
    inner_count = n - 4
    sources = (images_ref, texts_ref)

    def kind(k):
        return 1 if k < half else 0

    def part(k):
        return pl.ds(k % half * chunk, chunk)

    pieces, first = [], 0
    while first < half:
        count = min(max(first, 1), half - first)
        pieces.append((first, count))
        first += count
    pieces.append((half, half))

    def own_load(p):
        first, count = pieces[p]
        piece = pl.ds(first % half * chunk, count * chunk)
        i = kind(first)
        return pltpu.make_async_copy(sources[i].at[0, piece], own.at[i, piece], own_sem.at[p])

    def own_ready(k):
        for p, (first, _) in enumerate(pieces):
            if first == k:
                own_load(p).wait()

    def held_load(k):
        return pltpu.make_async_copy(
            sources[kind(k)].at[0, part(k)], held[k].at[me], load_sem.at[k]
        )

    small = [
        pltpu.make_async_copy(labels_in.at[0], labels_ref, small_sem.at[0]),
        pltpu.make_async_copy(partners_in, partners_ref, small_sem.at[1]),
    ]
    barrier = pltpu.get_barrier_semaphore()

    def signal(semaphore, **device):
        pl.semaphore_signal(semaphore, inc=1, device_id=device, device_id_type=MESH)

    own_load(0).start()

    @pl.when(inner)
    def _():
        for other in (across, near, far):
            for c in range(2):
                signal(barrier, blk=2 * other + c)

    @pl.when(outer)
    def _():
        for c in range(2):
            signal(barrier, blk=2 * beside + c)

    signal(barrier, blk=sibling)

    @pl.when(hub)
    def _():
        for step in range(1, groups):
            signal(barrier, grp=lax.rem(grp + step, groups))

    for p in range(1, len(pieces)):
        own_load(p).start()
    for copy in small:
        copy.start()
    pl.when(hub)(lambda: pl.semaphore_wait(barrier, 5 + groups - 1))
    pl.when(jnp.logical_not(hub))(lambda: pl.semaphore_wait(barrier, 5))

    def remote(src, dst, send, recv, **device):
        return pltpu.make_async_remote_copy(
            src_ref=src, dst_ref=dst, send_sem=send, recv_sem=recv,
            device_id=device, device_id_type=MESH,
        )

    def send_rows(k, target, send):
        return remote(
            own.at[kind(k), part(k)], held[k].at[me], send, recv_sem.at[k], blk=target
        )

    def rows_arrived(k):
        block = held[k].at[pl.ds(0, n - 1)]
        return remote(block, block, send_sem.at[0], recv_sem.at[k], blk=sibling)

    def all_rows_sent(send):
        return remote(own, own, send, recv_sem.at[0], blk=sibling)

    def half_rows_sent(send):
        return remote(own.at[0], own.at[0], send, recv_sem.at[0], blk=sibling)

    def forward(k):
        return remote(held[k], held[k], forward_sem.at[k], forwarded_sem.at[k], blk=sibling)

    def slot_copy(k, c):
        return remote(
            stage.at[k // 2, c], slots.at[k], slot_send, slot_recv.at[k], blk=2 * near + c
        )

    def outer_loss_copy():
        return remote(
            outer_loss.at[0], outer_loss.at[1], outer_send, outer_recv, blk=2 * beside + core
        )

    def loss_copy(index, blk, group):
        slot = loss_in.at[index]
        return remote(slot, slot, loss_send, loss_recv, blk=blk, grp=group)

    def losses_arrived(count):
        slot = loss_in.at[pl.ds(0, count)]
        return remote(slot, slot, loss_send, loss_recv, blk=sibling)

    def losses_sent():
        return remote(loss_sent, loss_sent, loss_send, loss_recv, blk=sibling)

    def own_pair():
        logits = scale_ref[...] * rows_dot(own[1], own[0]) + bias_ref[...]
        positive = lax.broadcasted_iota(jnp.int32, logits.shape, 0) == labels_ref[...]
        signed = jnp.where(positive, -1.0, 1.0)
        weight, terms = logistic_terms(signed * logits)
        weight = (signed * weight).astype(jnp.bfloat16)
        loss_sum[...] = fold(terms)
        image_acc[0] = weight_dot(weight, own[1])
        text_acc[0] = jnp.dot(weight, own[0], preferred_element_type=jnp.float32)

    def their_weight(found, i):
        logits = scale_ref[...] * rows_dot(found, own[1 - i]) + bias_ref[...]
        weight, terms = logistic_terms(logits)
        if i == 1:
            loss_sum[...] += fold(terms)
        return weight.astype(jnp.bfloat16)

    def add_pairs(found, i):
        acc = image_acc if i == 1 else text_acc
        acc[0] += weight_dot(their_weight(found, i), found)

    def leave_pairs(found, i):
        tail_weight[...] = their_weight(found, i)
        tail_rows[...] = found

    def joined(parts):
        return jnp.concatenate(parts, axis=0)

    def loss_total():
        total = loss_in[0]
        for at in range(1, inner_count * groups):
            total = total + loss_in[at]
        loss_ref[...] = total

    def in_groups(first, last):
        return [
            list(range(k, min(k + GROUP_CHUNKS, last)))
            for k in range(first, last, GROUP_CHUNKS)
        ]

    text_groups = in_groups(0, half)
    image_groups = in_groups(half, chunks - 1)
    loss_group = image_groups[-2]

    @pl.when(outer)
    def _():
        def send_chunks(first, last):
            for k in range(first, min(last, chunks)):
                send_rows(k, 2 * across + k % 2, send_sem.at[0]).start()
                send_rows(k, 2 * beside + k % 2, send_sem.at[1]).start()

        for k in range(AHEAD_CHUNKS):
            own_ready(k)
            send_chunks(k, k + 1)
        for k in range(AHEAD_CHUNKS, chunks):
            own_ready(k)
        for other in (beside, across):
            signal(seen_outer, blk=2 * other + core)
        for copy in small:
            copy.wait()
        own_pair()

        def slot_rows(members):
            for k in members:
                slot_copy(k, 0).wait_recv()
                send_chunks(k + AHEAD_CHUNKS, k + AHEAD_CHUNKS + 1)
            return joined([slots[k, r] for r in range(rounds) for k in members])

        for members in text_groups:
            add_pairs(slot_rows(members), 1)
            if members[0] == 0:
                @pl.when(hub)
                def _():
                    pl.semaphore_wait(seen_line, 1)
                    for step in range(1, groups):
                        signal(seen_group, grp=lax.rem(grp + step, groups))
                    pl.semaphore_wait(seen_group, groups - 1)
                    for other in (beside, across):
                        signal(seen_all, blk=2 * other + core)

        outer_loss[0] = jnp.sum(loss_sum[...], axis=0, keepdims=True)
        outer_loss_copy().start()
        image_acc[0] = scale_ref[...] * image_acc[0]
        for members in image_groups:
            add_pairs(slot_rows(members), 0)
        outer_loss_copy().wait_send()
        losses_arrived(inner_count * groups).wait_recv()
        loss_total()
        all_rows_sent(send_sem.at[0]).wait_send()
        all_rows_sent(send_sem.at[1]).wait_send()
        leave_pairs(slot_rows([chunks - 1]), 0)

    @pl.when(inner)
    def _():
        for k in range(chunks):
            own_ready(k)
            send_rows(k, 2 * across + k % 2, send_sem.at[0]).start()
            pl.when(core != k % 2)(
                lambda k=k: send_rows(k, sibling, sibling_sem).start()
            )
        for k in range(chunks):
            pl.when(core == k % 2)(lambda k=k: held_load(k).start())
        for copy in small:
            copy.wait()
        own_pair()

        def select(k):
            held_load(k).wait()
            rows_arrived(k).wait_recv()
            for c in range(2):
                for r in range(rounds):
                    stage[k // 2, c, r] = held[k][partners_ref[r, 2 * near + c]]
                slot_copy(k, c).start()
            forward(k).start()

        def held_rows(members):
            for c in range(2):
                @pl.when(core == c)
                def _():
                    for k in members:
                        if k % 2 == c:
                            select(k)
                    for k in members:
                        if k % 2 != c:
                            forward(k).wait_recv()
            return joined([held[k][partners_ref[r, me]] for r in range(rounds) for k in members])

        def send_loss():
            outer_loss_copy().wait_recv()
            pl.semaphore_wait(seen_all, 1)
            index = grp * inner_count + me - 2
            loss_in[index] = jnp.sum(loss_sum[...], axis=0, keepdims=True) + outer_loss[1]
            for group in range(groups):
                for blk in (0, 1, n - 2, n - 1):
                    loss_copy(index, blk, group).start()
            for step in range(groups):
                for hop in range(inner_count):
                    if step + hop > 0:
                        blk = 2 + lax.rem(me - 2 + hop, inner_count)
                        loss_copy(index, blk, lax.rem(grp + step, groups)).start()

        for members in text_groups:
            add_pairs(held_rows(members), 1)
            if members[0] == 0:
                pl.semaphore_wait(seen_outer, 2)
                pl.when(low)(lambda: signal(seen_line, blk=2 * near + core))
        image_acc[0] = scale_ref[...] * image_acc[0]
        for members in image_groups:
            add_pairs(held_rows(members), 0)
            if members == loss_group:
                send_loss()
        losses_sent().wait_send()
        losses_arrived(inner_count * groups - 1).wait_recv()
        loss_total()
        for k in range(chunks - 2):
            pl.when(core == k % 2)(lambda k=k: forward(k).wait_send())
        leave_pairs(held_rows([chunks - 1]), 0)
        for k in range(chunks - 2, chunks):
            pl.when(core == k % 2)(lambda k=k: forward(k).wait_send())
        all_rows_sent(send_sem.at[0]).wait_send()
        half_rows_sent(sibling_sem).wait_send()
        remote(stage, stage, slot_send, slot_recv.at[0], blk=sibling).wait_send()


def finish_kernel(
    image_count, scale_ref, image_in, text_in, weight, tail, loss_in,
    image_out, text_out, loss_out, ready, loss_cell, image_sem, sems, loss_sem,
):
    rows = text_in.shape[1]
    copies = [pltpu.make_async_copy(image_in, image_out, image_sem)]
    copies[-1].start()
    for at in range(FINISH_STEPS):
        part = pl.ds(at * (rows // FINISH_STEPS), rows // FINISH_STEPS)
        total = text_in[0, part] + weight_dot(weight[:, part], tail[...])
        ready[part] = scale_ref[...] * total
        copies.append(pltpu.make_async_copy(ready.at[part], text_out.at[0, part], sems.at[at]))
        copies[-1].start()
    loss_cell[0, 0] = jnp.sum(loss_in[...]) / jnp.float32(image_count)
    copies.append(pltpu.make_async_copy(loss_cell, loss_out, loss_sem))
    copies[-1].start()
    for copy in copies:
        copy.wait()


def keep(array):
    return pltpu.with_memory_space_constraint(array, pltpu.HBM)


def line_body(n, groups, images, texts, labels, partners, logit_scale, logit_bias):
    _, rows, width = images.shape
    rounds = partners.shape[0]
    chunk = CHUNK_ROWS
    chunks = 2 * rows // chunk
    vmem = pl.BlockSpec(memory_space=pltpu.VMEM)
    smem = pl.BlockSpec(memory_space=pltpu.SMEM)
    hbm = pl.BlockSpec(memory_space=pl.ANY)
    dma = pltpu.SemaphoreType.DMA
    regular = pltpu.SemaphoreType.REGULAR
    grad = jax.ShapeDtypeStruct(images.shape, jnp.float32)
    inner_count = n - 4
    image_sum, text_sum, weight, tail, loss_sum = pl.pallas_call(
        functools.partial(exchange_kernel, n, groups, rounds, chunk),
        out_shape=(
            grad, grad,
            jax.ShapeDtypeStruct((rounds * chunk, rows), jnp.bfloat16),
            jax.ShapeDtypeStruct((rounds * chunk, width), images.dtype),
            jax.ShapeDtypeStruct((1, 128), jnp.float32),
        ),
        in_specs=[hbm, smem, smem, hbm, hbm, hbm],
        out_specs=(vmem,) * 5,
        scratch_shapes=[
            pltpu.SMEM((rounds, n), jnp.int32),
            pltpu.VMEM((1, rows), jnp.int32),
            dma((2,)),
            pltpu.VMEM((2, rows, width), images.dtype),
            pltpu.VMEM((chunks // 2, 2, rounds, chunk, width), images.dtype),
            pltpu.VMEM((chunks, rounds, chunk, width), images.dtype),
            pltpu.VMEM((8, 128), jnp.float32),
            pltpu.VMEM((2, 1, 128), jnp.float32),
            pltpu.VMEM((inner_count * groups, 1, 128), jnp.float32),
            pltpu.VMEM((n * groups - 1, 1, 128), jnp.float32),
            dma((chunks,)),
            dma((chunks,)),
            dma((chunks,)),
            dma((2,)),
            dma,
            dma((chunks,)),
            dma((chunks,)),
            dma,
            dma((chunks,)),
            dma,
            dma,
            dma,
            dma,
            regular,
            regular,
            regular,
            regular,
        ]
        + [pltpu.VMEM((n, chunk, width), images.dtype) for _ in range(chunks)],
        compiler_params=pltpu.CompilerParams(
            collective_id=0, has_side_effects=True, vmem_limit_bytes=VMEM_LIMIT
        ),
    )(
        keep(partners), logit_scale, logit_bias,
        keep(labels), keep(images), keep(texts),
    )
    image_grad, text_grad, loss = pl.pallas_call(
        functools.partial(finish_kernel, n * groups * rows),
        out_shape=(grad, grad, jax.ShapeDtypeStruct((1, 1), jnp.float32)),
        in_specs=[smem] + [vmem] * 5,
        out_specs=(hbm, hbm, hbm),
        scratch_shapes=[
            pltpu.VMEM((rows, width), jnp.float32),
            pltpu.SMEM((1, 1), jnp.float32),
            dma,
            dma((FINISH_STEPS,)),
            dma,
        ],
        compiler_params=pltpu.CompilerParams(vmem_limit_bytes=FINISH_LIMIT),
    )(logit_scale, image_sum, text_sum, weight, tail, loss_sum)
    return image_grad, text_grad, loss.reshape(())


def solution(mesh):
    in_specs = (P("grp", "blk", None), P("grp", "blk", None), P("grp", "blk", None), P(), P(), P())
    out_specs = (P("grp", "blk", None), P("grp", "blk", None), P())
    n, groups = mesh.shape["blk"], mesh.shape["grp"]

    def body(images, texts, labels, partners, logit_scale, logit_bias):
        _, rows, width = images.shape
        rounds = partners.shape[0]
        block = 2 * rows * width * images.dtype.itemsize
        needed = block * (n + 3 * rounds + 1) + 2 * rows * width * 4
        fits = needed <= VMEM_BUDGET and n == 2 * LINE_CHIPS and groups > 1
        chunked = rows % (2 * CHUNK_ROWS * GROUP_CHUNKS) == 0 and rows % 128 == 0
        if fits and chunked and width % 128 == 0:
            return line_body(
                n, groups, images, texts, labels, partners, logit_scale, logit_bias
            )
        return spread_body(images, texts, labels, partners, logit_scale, logit_bias)

    return jax.shard_map(body, mesh=mesh, in_specs=in_specs, out_specs=out_specs, check_vma=False)
```

```python
import functools
import jax
import jax.numpy as jnp
from jax import lax
from jax.experimental import pallas as pl
from jax.experimental.pallas import tpu as pltpu
from jax.sharding import PartitionSpec as P

MESH = pl.DeviceIdType.MESH
CHUNK_ROWS = 16
GROUP_CHUNKS = 4
AHEAD_CHUNKS = 8
LINE_CHIPS = 4
VMEM_BUDGET = 48 * 1024 * 1024
VMEM_LIMIT = 32 * 1024 * 1024
FINISH_LIMIT = 16 * 1024 * 1024
FINISH_STEPS = 2


def block_weights(image_rows, text_rows, positive, logit_scale, logit_bias):
    logits = (
        logit_scale * jnp.dot(image_rows, text_rows.T, preferred_element_type=jnp.float32)
        + logit_bias
    )
    signed = jnp.where(positive, jnp.float32(1.0), jnp.float32(-1.0))
    loss_sum = jnp.sum(jax.nn.softplus(-signed * logits))
    weight = (-signed * jax.nn.sigmoid(-signed * logits)).astype(jnp.bfloat16)
    return (loss_sum, weight)


def regroup(received, partner_row):
    row_count, width = received.shape
    devices = partner_row.shape[0]
    pieces = received.reshape(row_count, devices, width // devices)
    pieces = jnp.take(pieces, partner_row, axis=1)
    return pieces.reshape(row_count, width)


def spread_body(images, texts, labels, partners, logit_scale, logit_bias):
    own_images = images[0]
    own_texts = texts[0]
    row_count = own_images.shape[0]
    columns = jnp.arange(row_count, dtype=jnp.int32)
    positive = labels[0, 0][:, None] == columns[None, :]
    nothing = jnp.zeros((row_count, row_count), dtype=bool)
    loss_sum, weight = block_weights(own_images, own_texts, positive, logit_scale, logit_bias)
    image_grad = logit_scale * jnp.dot(weight, own_texts, preferred_element_type=jnp.float32)
    text_grad = logit_scale * jnp.dot(weight.T, own_images, preferred_element_type=jnp.float32)
    for round_index in range(partners.shape[0]):
        partner_row = partners[round_index]
        spread_images, spread_texts = (
            lax.all_to_all(own_images, "blk", split_axis=1, concat_axis=1, tiled=True),
            lax.all_to_all(own_texts, "blk", split_axis=1, concat_axis=1, tiled=True),
        )
        their_images, their_texts = (
            lax.all_to_all(
                regroup(spread_images, partner_row), "blk", split_axis=1, concat_axis=1, tiled=True
            ),
            lax.all_to_all(
                regroup(spread_texts, partner_row), "blk", split_axis=1, concat_axis=1, tiled=True
            ),
        )
        round_loss, weight = block_weights(
            own_images, their_texts, nothing, logit_scale, logit_bias
        )
        image_grad = image_grad + logit_scale * jnp.dot(
            weight, their_texts, preferred_element_type=jnp.float32
        )
        _, mirror = block_weights(
            their_images, own_texts, nothing, logit_scale, logit_bias
        )
        text_grad = text_grad + logit_scale * jnp.dot(
            mirror.T, their_images, preferred_element_type=jnp.float32
        )
        loss_sum = loss_sum + round_loss
    loss_all = lax.psum(loss_sum, ("blk", "grp"))
    image_count = lax.axis_size("blk") * lax.axis_size("grp") * row_count
    loss = loss_all / jnp.float32(image_count)
    return (image_grad[None], text_grad[None], loss)


def logistic_terms(value):
    small = jnp.exp(-jnp.abs(value))
    inverse = 1.0 / (1.0 + small)
    weight = jnp.where(value >= 0, inverse, small * inverse)
    return weight, jnp.maximum(value, 0.0) + jnp.log1p(small)


def rows_dot(rows, own):
    return lax.dot_general(rows, own, (((1,), (1,)), ((), ())), preferred_element_type=jnp.float32)


def weight_dot(weight, rows):
    return lax.dot_general(
        weight, rows, (((0,), (0,)), ((), ())), preferred_element_type=jnp.float32
    )


def fold(terms):
    rows, columns = terms.shape
    total = jnp.sum(terms.reshape(rows // 8, 8, columns), axis=0)
    return sum(total[:, c : c + 128] for c in range(0, columns, 128))


def exchange_kernel(
    n, groups, rounds, chunk,
    partners_in, scale_ref, bias_ref, labels_in, images_ref, texts_ref,
    image_acc, text_acc, tail_weight, tail_rows, loss_ref,
    partners_ref, labels_ref, small_sem, own, stage, slots, loss_sum, outer_loss, loss_in, loss_sent,
    own_sem, load_sem, recv_sem, send_sem, sibling_sem, forward_sem, forwarded_sem,
    slot_send, slot_recv, outer_send, outer_recv, loss_send, loss_recv,
    seen_outer, seen_line, seen_group, seen_all, *held,
):
    rows = own.shape[1]
    half = rows // chunk
    chunks = 2 * half
    chips = n // 2
    me = lax.axis_index("blk")
    grp = lax.axis_index("grp")
    chip = lax.div(me, 2)
    core = lax.rem(me, 2)
    sibling = me + 1 - 2 * core
    low = chip < chips // 2
    outer = jnp.logical_or(chip == 0, chip == chips - 1)
    inner = jnp.logical_not(outer)
    hub = chip == 0
    near = jnp.where(low, 0, chips - 1)
    far = chips - 1 - near
    beside = jnp.where(low, 1, chips - 2)
    across = chips - 1 - beside
    inner_count = n - 4
    sources = (images_ref, texts_ref)

    def kind(k):
        return 1 if k < half else 0

    def part(k):
        return pl.ds(k % half * chunk, chunk)

    pieces, first = [], 0
    while first < half:
        count = min(max(first, 1), half - first)
        pieces.append((first, count))
        first += count
    pieces.append((half, half))

    def own_load(p):
        first, count = pieces[p]
        piece = pl.ds(first % half * chunk, count * chunk)
        i = kind(first)
        return pltpu.make_async_copy(sources[i].at[0, piece], own.at[i, piece], own_sem.at[p])

    def own_ready(k):
        for p, (first, _) in enumerate(pieces):
            if first == k:
                own_load(p).wait()

    def held_load(k):
        return pltpu.make_async_copy(
            sources[kind(k)].at[0, part(k)], held[k].at[me], load_sem.at[k]
        )

    small = [
        pltpu.make_async_copy(labels_in.at[0], labels_ref, small_sem.at[0]),
        pltpu.make_async_copy(partners_in, partners_ref, small_sem.at[1]),
    ]
    barrier = pltpu.get_barrier_semaphore()

    def signal(semaphore, **device):
        pl.semaphore_signal(semaphore, inc=1, device_id=device, device_id_type=MESH)

    own_load(0).start()

    @pl.when(inner)
    def _():
        for other in (across, near, far):
            for c in range(2):
                signal(barrier, blk=2 * other + c)

    @pl.when(outer)
    def _():
        for c in range(2):
            signal(barrier, blk=2 * beside + c)

    signal(barrier, blk=sibling)

    @pl.when(hub)
    def _():
        for step in range(1, groups):
            signal(barrier, grp=lax.rem(grp + step, groups))

    for p in range(1, len(pieces)):
        own_load(p).start()
    for copy in small:
        copy.start()
    pl.when(hub)(lambda: pl.semaphore_wait(barrier, 5 + groups - 1))
    pl.when(jnp.logical_not(hub))(lambda: pl.semaphore_wait(barrier, 5))

    def remote(src, dst, send, recv, **device):
        return pltpu.make_async_remote_copy(
            src_ref=src, dst_ref=dst, send_sem=send, recv_sem=recv,
            device_id=device, device_id_type=MESH,
        )

    def send_rows(k, target, send):
        return remote(
            own.at[kind(k), part(k)], held[k].at[me], send, recv_sem.at[k], blk=target
        )

    def rows_arrived(k):
        block = held[k].at[pl.ds(0, n - 1)]
        return remote(block, block, send_sem.at[0], recv_sem.at[k], blk=sibling)

    def all_rows_sent(send):
        return remote(own, own, send, recv_sem.at[0], blk=sibling)

    def half_rows_sent(send):
        return remote(own.at[0], own.at[0], send, recv_sem.at[0], blk=sibling)

    def forward(k):
        return remote(held[k], held[k], forward_sem.at[k], forwarded_sem.at[k], blk=sibling)

    def slot_copy(k, c):
        return remote(
            stage.at[k // 2, c], slots.at[k], slot_send, slot_recv.at[k], blk=2 * near + c
        )

    def outer_loss_copy():
        return remote(
            outer_loss.at[0], outer_loss.at[1], outer_send, outer_recv, blk=2 * beside + core
        )

    def loss_copy(index, blk, group):
        slot = loss_in.at[index]
        return remote(slot, slot, loss_send, loss_recv, blk=blk, grp=group)

    def losses_arrived(count):
        slot = loss_in.at[pl.ds(0, count)]
        return remote(slot, slot, loss_send, loss_recv, blk=sibling)

    def losses_sent():
        return remote(loss_sent, loss_sent, loss_send, loss_recv, blk=sibling)

    def own_pair():
        logits = scale_ref[...] * rows_dot(own[1], own[0]) + bias_ref[...]
        positive = lax.broadcasted_iota(jnp.int32, logits.shape, 0) == labels_ref[...]
        signed = jnp.where(positive, -1.0, 1.0)
        weight, terms = logistic_terms(signed * logits)
        weight = (signed * weight).astype(jnp.bfloat16)
        loss_sum[...] = fold(terms)
        image_acc[0] = weight_dot(weight, own[1])
        text_acc[0] = jnp.dot(weight, own[0], preferred_element_type=jnp.float32)

    def their_weight(found, i):
        logits = scale_ref[...] * rows_dot(found, own[1 - i]) + bias_ref[...]
        weight, terms = logistic_terms(logits)
        if i == 1:
            loss_sum[...] += fold(terms)
        return weight.astype(jnp.bfloat16)

    def add_pairs(found, i):
        acc = image_acc if i == 1 else text_acc
        acc[0] += weight_dot(their_weight(found, i), found)

    def leave_pairs(found, i):
        tail_weight[...] = their_weight(found, i)
        tail_rows[...] = found

    def joined(parts):
        return jnp.concatenate(parts, axis=0)

    def loss_total():
        total = loss_in[0]
        for at in range(1, inner_count * groups):
            total = total + loss_in[at]
        loss_ref[...] = total

    def in_groups(first, last):
        return [
            list(range(k, min(k + GROUP_CHUNKS, last)))
            for k in range(first, last, GROUP_CHUNKS)
        ]

    text_groups = in_groups(0, half)
    image_groups = in_groups(half, chunks - 1)
    loss_group = image_groups[-2]

    @pl.when(outer)
    def _():
        def send_chunks(first, last):
            for k in range(first, min(last, chunks)):
                send_rows(k, 2 * across + k % 2, send_sem.at[0]).start()
                send_rows(k, 2 * beside + k % 2, send_sem.at[1]).start()

        for k in range(AHEAD_CHUNKS):
            own_ready(k)
            send_chunks(k, k + 1)
        for k in range(AHEAD_CHUNKS, chunks):
            own_ready(k)
        for other in (beside, across):
            signal(seen_outer, blk=2 * other + core)
        for copy in small:
            copy.wait()
        own_pair()

        def slot_rows(members):
            for k in members:
                slot_copy(k, 0).wait_recv()
                send_chunks(k + AHEAD_CHUNKS, k + AHEAD_CHUNKS + 1)
            return joined([slots[k, r] for r in range(rounds) for k in members])

        for members in text_groups:
            add_pairs(slot_rows(members), 1)
            if members[0] == 0:
                @pl.when(hub)
                def _():
                    pl.semaphore_wait(seen_line, 1)
                    for step in range(1, groups):
                        signal(seen_group, grp=lax.rem(grp + step, groups))
                    pl.semaphore_wait(seen_group, groups - 1)
                    for other in (beside, across):
                        signal(seen_all, blk=2 * other + core)

        outer_loss[0] = jnp.sum(loss_sum[...], axis=0, keepdims=True)
        outer_loss_copy().start()
        image_acc[0] = scale_ref[...] * image_acc[0]
        for members in image_groups:
            add_pairs(slot_rows(members), 0)
        outer_loss_copy().wait_send()
        losses_arrived(inner_count * groups).wait_recv()
        loss_total()
        all_rows_sent(send_sem.at[0]).wait_send()
        all_rows_sent(send_sem.at[1]).wait_send()
        leave_pairs(slot_rows([chunks - 1]), 0)

    @pl.when(inner)
    def _():
        for k in range(chunks):
            own_ready(k)
            send_rows(k, 2 * across + k % 2, send_sem.at[0]).start()
            pl.when(core != k % 2)(
                lambda k=k: send_rows(k, sibling, sibling_sem).start()
            )
        for k in range(chunks):
            pl.when(core == k % 2)(lambda k=k: held_load(k).start())
        for copy in small:
            copy.wait()
        own_pair()

        def select(k):
            held_load(k).wait()
            rows_arrived(k).wait_recv()
            for c in range(2):
                for r in range(rounds):
                    stage[k // 2, c, r] = held[k][partners_ref[r, 2 * near + c]]
                slot_copy(k, c).start()
            forward(k).start()

        def held_rows(members):
            for c in range(2):
                @pl.when(core == c)
                def _():
                    for k in members:
                        if k % 2 == c:
                            select(k)
                    for k in members:
                        if k % 2 != c:
                            forward(k).wait_recv()
            return joined([held[k][partners_ref[r, me]] for r in range(rounds) for k in members])

        def send_loss():
            outer_loss_copy().wait_recv()
            pl.semaphore_wait(seen_all, 1)
            index = grp * inner_count + me - 2
            loss_in[index] = jnp.sum(loss_sum[...], axis=0, keepdims=True) + outer_loss[1]
            for group in range(groups):
                for blk in (0, 1, n - 2, n - 1):
                    loss_copy(index, blk, group).start()
            for step in range(groups):
                for hop in range(inner_count):
                    if step + hop > 0:
                        blk = 2 + lax.rem(me - 2 + hop, inner_count)
                        loss_copy(index, blk, lax.rem(grp + step, groups)).start()

        for members in text_groups:
            add_pairs(held_rows(members), 1)
            if members[0] == 0:
                pl.semaphore_wait(seen_outer, 2)
                pl.when(low)(lambda: signal(seen_line, blk=2 * near + core))
        image_acc[0] = scale_ref[...] * image_acc[0]
        for members in image_groups:
            add_pairs(held_rows(members), 0)
            if members == loss_group:
                send_loss()
        losses_sent().wait_send()
        losses_arrived(inner_count * groups - 1).wait_recv()
        loss_total()
        for k in range(chunks - 2):
            pl.when(core == k % 2)(lambda k=k: forward(k).wait_send())
        leave_pairs(held_rows([chunks - 1]), 0)
        for k in range(chunks - 2, chunks):
            pl.when(core == k % 2)(lambda k=k: forward(k).wait_send())
        all_rows_sent(send_sem.at[0]).wait_send()
        half_rows_sent(sibling_sem).wait_send()
        remote(stage, stage, slot_send, slot_recv.at[0], blk=sibling).wait_send()


def finish_kernel(
    image_count, scale_ref, image_in, text_in, weight, tail, loss_in,
    image_out, text_out, loss_out, ready, loss_cell, image_sem, sems, loss_sem,
):
    rows = text_in.shape[1]
    copies = [pltpu.make_async_copy(image_in, image_out, image_sem)]
    copies[-1].start()
    for at in range(FINISH_STEPS):
        part = pl.ds(at * (rows // FINISH_STEPS), rows // FINISH_STEPS)
        total = text_in[0, part] + weight_dot(weight[:, part], tail[...])
        ready[part] = scale_ref[...] * total
        copies.append(pltpu.make_async_copy(ready.at[part], text_out.at[0, part], sems.at[at]))
        copies[-1].start()
    loss_cell[0, 0] = jnp.sum(loss_in[...]) / jnp.float32(image_count)
    copies.append(pltpu.make_async_copy(loss_cell, loss_out, loss_sem))
    copies[-1].start()
    for copy in copies:
        copy.wait()


def keep(array):
    return pltpu.with_memory_space_constraint(array, pltpu.HBM)


def line_body(n, groups, images, texts, labels, partners, logit_scale, logit_bias):
    _, rows, width = images.shape
    rounds = partners.shape[0]
    chunk = CHUNK_ROWS
    chunks = 2 * rows // chunk
    vmem = pl.BlockSpec(memory_space=pltpu.VMEM)
    smem = pl.BlockSpec(memory_space=pltpu.SMEM)
    hbm = pl.BlockSpec(memory_space=pl.ANY)
    dma = pltpu.SemaphoreType.DMA
    regular = pltpu.SemaphoreType.REGULAR
    grad = jax.ShapeDtypeStruct(images.shape, jnp.float32)
    inner_count = n - 4
    image_sum, text_sum, weight, tail, loss_sum = pl.pallas_call(
        functools.partial(exchange_kernel, n, groups, rounds, chunk),
        out_shape=(
            grad, grad,
            jax.ShapeDtypeStruct((rounds * chunk, rows), jnp.bfloat16),
            jax.ShapeDtypeStruct((rounds * chunk, width), images.dtype),
            jax.ShapeDtypeStruct((1, 128), jnp.float32),
        ),
        in_specs=[hbm, smem, smem, hbm, hbm, hbm],
        out_specs=(vmem,) * 5,
        scratch_shapes=[
            pltpu.SMEM((rounds, n), jnp.int32),
            pltpu.VMEM((1, rows), jnp.int32),
            dma((2,)),
            pltpu.VMEM((2, rows, width), images.dtype),
            pltpu.VMEM((chunks // 2, 2, rounds, chunk, width), images.dtype),
            pltpu.VMEM((chunks, rounds, chunk, width), images.dtype),
            pltpu.VMEM((8, 128), jnp.float32),
            pltpu.VMEM((2, 1, 128), jnp.float32),
            pltpu.VMEM((inner_count * groups, 1, 128), jnp.float32),
            pltpu.VMEM((n * groups - 1, 1, 128), jnp.float32),
            dma((chunks,)),
            dma((chunks,)),
            dma((chunks,)),
            dma((2,)),
            dma,
            dma((chunks,)),
            dma((chunks,)),
            dma,
            dma((chunks,)),
            dma,
            dma,
            dma,
            dma,
            regular,
            regular,
            regular,
            regular,
        ]
        + [pltpu.VMEM((n, chunk, width), images.dtype) for _ in range(chunks)],
        compiler_params=pltpu.CompilerParams(
            collective_id=0, has_side_effects=True, vmem_limit_bytes=VMEM_LIMIT
        ),
    )(
        keep(partners), logit_scale, logit_bias,
        keep(labels), keep(images), keep(texts),
    )
    image_grad, text_grad, loss = pl.pallas_call(
        functools.partial(finish_kernel, n * groups * rows),
        out_shape=(grad, grad, jax.ShapeDtypeStruct((1, 1), jnp.float32)),
        in_specs=[smem] + [vmem] * 5,
        out_specs=(hbm, hbm, hbm),
        scratch_shapes=[
            pltpu.VMEM((rows, width), jnp.float32),
            pltpu.SMEM((1, 1), jnp.float32),
            dma,
            dma((FINISH_STEPS,)),
            dma,
        ],
        compiler_params=pltpu.CompilerParams(vmem_limit_bytes=FINISH_LIMIT),
    )(logit_scale, image_sum, text_sum, weight, tail, loss_sum)
    return image_grad, text_grad, loss.reshape(())


def solution(mesh):
    in_specs = (P("grp", "blk", None), P("grp", "blk", None), P("grp", "blk", None), P(), P(), P())
    out_specs = (P("grp", "blk", None), P("grp", "blk", None), P())
    n, groups = mesh.shape["blk"], mesh.shape["grp"]

    def body(images, texts, labels, partners, logit_scale, logit_bias):
        _, rows, width = images.shape
        rounds = partners.shape[0]
        block = 2 * rows * width * images.dtype.itemsize
        needed = block * (n + 3 * rounds + 1) + 2 * rows * width * 4
        fits = needed <= VMEM_BUDGET and n == 2 * LINE_CHIPS and groups > 1
        chunked = rows % (2 * CHUNK_ROWS * GROUP_CHUNKS) == 0 and rows % 128 == 0
        if fits and chunked and width % 128 == 0:
            return line_body(
                n, groups, images, texts, labels, partners, logit_scale, logit_bias
            )
        return spread_body(images, texts, labels, partners, logit_scale, logit_bias)

    return jax.shard_map(body, mesh=mesh, in_specs=in_specs, out_specs=out_specs, check_vma=False)
```
